128 devices in a mesh: dp: 1, b: 16 (over z, y), cp: 8 (over x, core).
Axes of the slice: x: 4, y: 4, z: 4, core: 2. Of those that a mesh axis runs over, the one named last changes fastest.
Arguments:
- x: bfloat16 [16, 2048, 2048], P(('dp', 'b'), 'cp')
- ids: int32 [16, 2048, 12], P(('dp', 'b'), 'cp')
- g_attn: bfloat16 [2048], replicated
- wq: bfloat16 [2048, 4096], replicated
- wk: bfloat16 [2048, 512], replicated
- wv: bfloat16 [2048, 512], replicated
- wo: bfloat16 [4096, 2048], replicated
- g_ffn: bfloat16 [2048], replicated
- w1: bfloat16 [2048, 6144], replicated
- w3: bfloat16 [2048, 6144], replicated
- w2: bfloat16 [6144, 2048], replicated
- g_moe: bfloat16 [2048], replicated
- wr: bfloat16 [2048, 192], replicated
- we_g: bfloat16 [128, 2048, 768], P(('b', 'cp'))
- we_u: bfloat16 [128, 2048, 768], P(('b', 'cp'))
- we_d: bfloat16 [128, 768, 2048], P(('b', 'cp'))
Outputs:
- output: bfloat16 [16, 2048, 2048], P(('dp', 'b'), 'cp')
All inputs are finite; a program needn't handle non-finite values.
Results may differ from the reference program's by a relative error of at most 0.00815073.
Values are sent between devices in bfloat16 or wider.
A program may use at most 1 GiB of HBM per device.

```python
import jax
import jax.numpy as jnp
from jax import lax

BATCH = 16
SEQ = 2048
D = 2048
HEADS = 32
KV_HEADS = 4
FF = 6144
EFF = 768
EXPERTS = 128
ZERO = 64
TOP = 12
NB = 16
NC = 8
HEAD = 128
ROPE = 64
QB = 64
EPS = 1e-6
THETA = 10000.0
RSCALE = 2.5


def rms_norm(x, g):
    xf = x.astype(jnp.float32)
    r = lax.rsqrt(jnp.mean(xf * xf, axis=-1, keepdims=True) + EPS)
    return (xf * r * g.astype(jnp.float32)).astype(jnp.bfloat16)


def rope(t, pos):
    half = ROPE // 2
    freq = THETA ** (-jnp.arange(half, dtype=jnp.float32) / half)
    ang = pos.astype(jnp.float32)[:, None] * freq[None, :]
    c = jnp.cos(ang)[:, None, :]
    s = jnp.sin(ang)[:, None, :]
    tf = t.astype(jnp.float32)
    t1 = tf[..., :half]
    t2 = tf[..., half:ROPE]
    out = jnp.concatenate([t1 * c - t2 * s, t2 * c + t1 * s, tf[..., ROPE:]], axis=-1)
    return out.astype(jnp.bfloat16)


def slot_rank(key):
    n = key.shape[0]
    order = jnp.argsort(key, stable=True)
    sk = key[order]
    first = jnp.searchsorted(sk, sk)
    return jnp.zeros((n,), jnp.int32).at[order].set((jnp.arange(n) - first).astype(jnp.int32))


def setup_inputs(seed: int = 0, part: int = 0) -> dict:
    kg = jax.random.key(seed)
    ks = jax.random.split(kg, 16)
    kp = jax.random.split(jax.random.fold_in(kg, part), 8)
    kz = jax.random.fold_in(kg, 7919)
    kzs = jax.random.split(kz, 2)
    kr = jax.random.split(jax.random.fold_in(kz, part + 1), 4)
    bd = BATCH // NB
    sd = SEQ // NC
    tl = bd * sd
    ns = tl * TOP
    cap = tl * TOP // EXPERTS
    nblk = NB * NC
    nseg = 16

    def w(k, shape, fan, sc):
        return (jax.random.normal(k, shape, jnp.float32) * (sc * fan ** -0.5)).astype(jnp.bfloat16)

    def gain(k):
        return (1.0 + 0.25 * jax.random.normal(k, (D,), jnp.float32)).astype(jnp.bfloat16)

    seg = jnp.arange(SEQ) * nseg // SEQ
    zs = jax.random.normal(kp[0], (BATCH, nseg, D), jnp.float32)
    noise = jax.random.normal(kp[1], (BATCH, SEQ, D), jnp.float32)
    x = (0.8 * zs[:, seg, :] + 0.6 * noise).astype(jnp.bfloat16)

    def limit(raw, zid):
        ffn = raw < EXPERTS
        rank = slot_rank(jnp.where(ffn, raw, EXPERTS))
        return jnp.where(ffn & (rank < cap), raw, zid)

    pop_sum = jnp.sum(jax.random.randint(kzs[0], (EXPERTS, 12), 0, 256), axis=1)
    pop_exp = jnp.clip((pop_sum - 1536) * 277 // 4096 + 64, 0, 127)
    pop_weight = (8 + (pop_exp & 7)) << (pop_exp >> 3)
    pop_cum = jnp.cumsum(pop_weight).astype(jnp.int32)
    zero_limit = jax.random.randint(kr[0], (nblk, tl, 1), 3277, 45876)
    zero_bits = (jax.random.bits(kr[1], (nblk, tl, TOP), jnp.uint32) >> 16).astype(jnp.int32)
    zero_pick = (zero_bits < zero_limit).reshape(nblk, ns)
    pick_draw = jax.random.randint(kr[2], (nblk, ns), 0, pop_cum[-1])
    ffn_id = jnp.minimum(jnp.searchsorted(pop_cum, pick_draw, side='right'), EXPERTS - 1).astype(jnp.int32)
    zero_id = EXPERTS + jax.random.randint(kr[3], (nblk, ns), 0, max(ZERO // 4, 1))
    raw = jnp.where(zero_pick, EXPERTS, ffn_id)
    blk = jax.vmap(limit)(raw, zero_id).astype(jnp.int32)
    ids = blk.reshape(NB, NC, bd, sd, TOP).transpose(0, 2, 1, 3, 4).reshape(BATCH, SEQ, TOP)
    return {
        'x': x,
        'ids': ids,
        'g_attn': gain(ks[0]),
        'wq': w(ks[1], (D, HEADS * HEAD), D, 2.0),
        'wk': w(ks[2], (D, KV_HEADS * HEAD), D, 1.0),
        'wv': w(ks[3], (D, KV_HEADS * HEAD), D, 1.0),
        'wo': w(ks[4], (HEADS * HEAD, D), HEADS * HEAD, 1.0),
        'g_ffn': gain(ks[5]),
        'w1': w(ks[6], (D, FF), D, 1.0),
        'w3': w(ks[7], (D, FF), D, 1.0),
        'w2': w(ks[8], (FF, D), FF, 1.0),
        'g_moe': gain(ks[9]),
        'wr': w(ks[10], (D, EXPERTS + ZERO), D, 1.5),
        'we_g': w(ks[11], (EXPERTS, D, EFF), D, 1.0),
        'we_u': w(ks[12], (EXPERTS, D, EFF), D, 1.0),
        'we_d': w(ks[13], (EXPERTS, EFF, D), EFF, 1.0),
    }


def reference(x, ids, g_attn, wq, wk, wv, wo, g_ffn, w1, w3, w2, g_moe, wr, we_g, we_u, we_d):
    S = x.shape[1]
    pos = jnp.arange(S)
    grp = HEADS // KV_HEADS
    scale = HEAD ** -0.5

    def proj(a, wt):
        return jnp.dot(a, wt, preferred_element_type=jnp.float32).astype(jnp.bfloat16)

    def attn_row(xr):
        n = rms_norm(xr, g_attn)
        q = rope(proj(n, wq).reshape(S, HEADS, HEAD), pos).reshape(S, KV_HEADS, grp, HEAD).astype(jnp.float32)
        k = rope(proj(n, wk).reshape(S, KV_HEADS, HEAD), pos).astype(jnp.float32)
        v = proj(n, wv).reshape(S, KV_HEADS, HEAD).astype(jnp.float32)

        def qblock(i):
            qb = lax.dynamic_slice_in_dim(q, i * QB, QB, axis=0)
            sc = jnp.einsum('qkgd,skd->kgqs', qb, k) * scale
            qp = i * QB + jnp.arange(QB)
            sc = jnp.where(qp[:, None] >= pos[None, :], sc, -jnp.inf)
            p = jax.nn.softmax(sc, axis=-1)
            return jnp.einsum('kgqs,skd->qkgd', p, v)

        o = lax.map(qblock, jnp.arange(S // QB)).reshape(S, HEADS * HEAD).astype(jnp.bfloat16)
        return proj(o, wo)

    a = lax.map(attn_row, x)
    y = (x.astype(jnp.float32) + a.astype(jnp.float32)).astype(jnp.bfloat16)

    def ffn_row(yr):
        z = rms_norm(yr, g_ffn)
        hh = (jax.nn.silu(jnp.dot(z, w1, preferred_element_type=jnp.float32)) * jnp.dot(z, w3, preferred_element_type=jnp.float32)).astype(jnp.bfloat16)
        return proj(hh, w2)

    f = lax.map(ffn_row, y)

    nt = BATCH * S
    N = nt * TOP
    gcap = N // EXPERTS
    u = rms_norm(x, g_moe).reshape(nt, D)
    logits = jnp.dot(u, wr, preferred_element_type=jnp.float32)
    idf = ids.reshape(nt, TOP)
    gate = RSCALE * jax.nn.softmax(jnp.take_along_axis(logits, idf, axis=1), axis=-1)
    e = idf.reshape(N)
    ffn = e < EXPERTS
    ek = jnp.where(ffn, e, EXPERTS)
    slot = jnp.where(ffn, ek * gcap + slot_rank(ek), EXPERTS * gcap)
    us = u[jnp.arange(N) // TOP]
    buf = jnp.zeros((EXPERTS * gcap, D), jnp.bfloat16).at[slot].set(us, mode='drop')

    def expert(args):
        xb, a1, a2, a3 = args
        hh = (jax.nn.silu(jnp.dot(xb, a1, preferred_element_type=jnp.float32)) * jnp.dot(xb, a2, preferred_element_type=jnp.float32)).astype(jnp.bfloat16)
        return proj(hh, a3)

    out = lax.map(expert, (buf.reshape(EXPERTS, gcap, D), we_g, we_u, we_d)).reshape(EXPERTS * gcap, D)
    got = out[jnp.minimum(slot, EXPERTS * gcap - 1)]
    val = jnp.where(ffn[:, None], got.astype(jnp.float32), us.astype(jnp.float32)).reshape(nt, TOP, D)
    m = jnp.einsum('tj,tjd->td', gate, val)
    h = y.astype(jnp.float32) + f.astype(jnp.float32) + m.reshape(BATCH, S, D)
    return h.astype(jnp.bfloat16)
```

```python
import functools

import jax
import jax.numpy as jnp
from jax import lax
from jax.experimental import pallas as pl
from jax.experimental.pallas import tpu as pltpu
from jax.sharding import PartitionSpec as P

HEAD = 128
ROPE = 64
EPS = 1e-6
THETA = 10000.0
RSCALE = 2.5
LOG2E = 1.4426950408889634
F32 = jnp.float32
BF16 = jnp.bfloat16


def rms_norm(x, g):
    xf = x.astype(F32)
    r = lax.rsqrt(jnp.mean(xf * xf, axis=-1, keepdims=True) + EPS)
    return (xf * r * g.astype(F32)).astype(BF16)


def proj(a, wt):
    return jnp.dot(a, wt, preferred_element_type=F32).astype(BF16)


def rope_tables(pos):
    half = ROPE // 2
    freq = THETA ** (-jnp.arange(half, dtype=F32) / half)
    ang = pos.astype(F32)[:, None] * freq[None, :]
    c, s = jnp.cos(ang), jnp.sin(ang)
    rest = jnp.ones((pos.shape[0], HEAD - ROPE), F32)
    return jnp.concatenate([c, c, rest], axis=-1), jnp.concatenate([-s, s, 0.0 * rest], axis=-1)


def rotate(t, c, s):
    half = ROPE // 2
    lane = lax.broadcasted_iota(jnp.int32, t.shape, 1)
    partner = jnp.where(lane < half, pltpu.roll(t, HEAD - half, 1), pltpu.roll(t, half, 1))
    return (t * c + partner * s).astype(BF16)


def vmem(n):
    return [pl.BlockSpec(memory_space=pltpu.VMEM)] * n


def front_kernel(x_ref, ids_ref, ga_ref, gm_ref, wk_ref, wv_ref, wr_ref, c_ref, s_ref, n_ref, u_ref, kv_ref, gate_ref, zero_ref, ex_ref, ext_ref):
    t, d = x_ref.shape
    nexp = ex_ref.shape[1]
    xf = x_ref[...].astype(F32)
    xr = xf * lax.rsqrt(jnp.mean(xf * xf, axis=-1, keepdims=True) + EPS)
    n = (xr * ga_ref[...].astype(F32)).astype(BF16)
    u = (xr * gm_ref[...].astype(F32)).astype(BF16)
    n_ref[...] = n
    u_ref[...] = u
    kd = wk_ref.shape[1]
    k = jnp.dot(n, wk_ref[...], preferred_element_type=F32).astype(BF16).astype(F32)
    for i in range(kd // HEAD):
        kv_ref[:, i * HEAD:(i + 1) * HEAD] = rotate(k[:, i * HEAD:(i + 1) * HEAD], c_ref[...], s_ref[...])
    kv_ref[:, kd:] = jnp.dot(n, wv_ref[...], preferred_element_type=F32).astype(BF16)
    logits = jnp.dot(u, wr_ref[...], preferred_element_type=F32)
    col = lax.broadcasted_iota(jnp.int32, logits.shape, 1)
    ids = ids_ref[...]
    mult = jnp.zeros(logits.shape, F32)
    for j in range(ids.shape[1]):
        mult += (ids[:, j:j + 1] == col).astype(F32)
    has = mult > 0.0
    top = jnp.max(jnp.where(has, logits, -jnp.inf), axis=-1, keepdims=True)
    e = jnp.where(has, mult * jnp.exp(jnp.minimum(logits - top, 0.0)), 0.0)
    gate = RSCALE * e / jnp.sum(e, axis=-1, keepdims=True)
    zero = jnp.sum(jnp.where(col >= nexp, gate, 0.0), axis=-1, keepdims=True)
    zero_ref[...] = jnp.broadcast_to(zero, zero_ref.shape)
    g = gate[:, :nexp]
    for i in range(3):
        part = g.astype(BF16)
        gate_ref[i * t:(i + 1) * t, :] = part
        g = g - part.astype(F32)
    here = has[:, :nexp]
    ti = lax.broadcasted_iota(jnp.int32, (t, t), 0)
    tj = lax.broadcasted_iota(jnp.int32, (t, t), 1)
    before = jnp.where(tj < ti, 1.0, 0.0).astype(BF16)
    rank = jnp.dot(before, jnp.where(here, 1.0, 0.0).astype(BF16), preferred_element_type=F32)
    rank = jnp.where(here, rank, -1.0)
    ex_ref[...] = rank.astype(BF16)
    ext_ref[...] = rank.T.astype(BF16)


def front(x, ids, ga, gm, wk, wv, wr, c, s, nexp):
    t, d = x.shape
    kd = wk.shape[1]
    shapes = [((t, d), BF16), ((t, d), BF16), ((t, 2 * kd), BF16), ((3 * t, nexp), BF16), ((t, HEAD), F32), ((t, nexp), BF16), ((nexp, t), BF16)]
    return pl.pallas_call(
        front_kernel,
        out_shape=[jax.ShapeDtypeStruct(*a) for a in shapes],
        in_specs=vmem(9),
        out_specs=vmem(7),
        cost_estimate=pl.CostEstimate(flops=2 * t * d * (2 * kd + wr.shape[1]), bytes_accessed=8 << 20, transcendentals=0),
        compiler_params=pltpu.CompilerParams(vmem_limit_bytes=48 << 20),
        name="front",
    )(x, ids, ga.reshape(1, d), gm.reshape(1, d), wk, wv, wr, c, s)


def dispatch_kernel(cap, ext_ref, u_ref, o_ref):
    rows = o_ref.shape[0]
    nexp = ext_ref.shape[0]
    r = pl.program_id(0) * rows + lax.broadcasted_iota(jnp.int32, (rows, nexp), 0)
    lo = cap * lax.broadcasted_iota(jnp.int32, (rows, nexp), 1)
    own = (r >= lo) & (r < lo + cap)
    rank = jnp.dot(jnp.where(own, 1.0, 0.0).astype(BF16), ext_ref[...], preferred_element_type=F32)
    slot = jnp.sum(jnp.where(own, (r - lo).astype(F32), 0.0), axis=-1, keepdims=True)
    sel = jnp.where(rank == slot, 1.0, 0.0).astype(BF16)
    o_ref[...] = jnp.dot(sel, u_ref[...], preferred_element_type=F32).astype(BF16)


def dispatch(ext, u, cap):
    nexp, t = ext.shape
    d = u.shape[1]
    rows = 16 * cap
    return pl.pallas_call(
        functools.partial(dispatch_kernel, cap),
        grid=(nexp * cap // rows,),
        out_shape=jax.ShapeDtypeStruct((nexp * cap, d), BF16),
        in_specs=[pl.BlockSpec((nexp, t), lambda i: (0, 0)), pl.BlockSpec((t, d), lambda i: (0, 0))],
        out_specs=pl.BlockSpec((rows, d), lambda i: (i, 0)),
        cost_estimate=pl.CostEstimate(flops=2 * nexp * cap * t * d, bytes_accessed=nexp * cap * d * 2, transcendentals=0),
        name="dispatch",
    )(ext, u)


def attend_kernel(grp, ci_ref, q_ref, k_ref, v_ref, c_ref, s_ref, o_ref, sc_ref):
    sd = q_ref.shape[0]
    ci = ci_ref[0]
    row = lax.broadcasted_iota(jnp.int32, (sd, sd), 0)
    colm = lax.broadcasted_iota(jnp.int32, (sd, sd), 1)
    for h in range(q_ref.shape[1] // HEAD):
        q = rotate(q_ref[:, h * HEAD:(h + 1) * HEAD].astype(F32), c_ref[...], s_ref[...])

        def score(j):
            kb = k_ref[pl.ds(pl.multiple_of(j * sd, sd), sd), :]
            return lax.dot_general(q, kb, (((1,), (1,)), ((), ())), preferred_element_type=F32) * (HEAD ** -0.5 * LOG2E)

        def fold(a, op):
            r = a[:, :HEAD]
            for i in range(1, sd // HEAD):
                r = op(r, a[:, i * HEAD:(i + 1) * HEAD])
            return r

        def first(j, m):
            sc = score(j)
            sc_ref[j] = sc
            return jnp.maximum(m, fold(sc, jnp.maximum))

        last = jnp.where(row >= colm, score(ci), -1e30)
        mx = lax.fori_loop(0, ci, first, fold(last, jnp.maximum))
        mx = jnp.max(mx, axis=-1, keepdims=True)

        def weigh(sc, j, den, acc):
            p = jnp.exp2(sc - mx)
            vb = v_ref[pl.ds(pl.multiple_of(j * sd, sd), sd), :]
            return den + fold(p, jnp.add), acc + jnp.dot(p.astype(BF16), vb, preferred_element_type=F32)

        zero = jnp.zeros((sd, HEAD), F32)
        den, acc = weigh(last, ci, zero, zero)
        den, acc = lax.fori_loop(0, ci, lambda j, st: weigh(sc_ref[j], j, *st), (den, acc))
        o_ref[:, h * HEAD:(h + 1) * HEAD] = (acc / jnp.sum(den, axis=-1, keepdims=True)).astype(BF16)


def attention(ci, q, kv, c, s, ncp):
    sd, qd = q.shape
    kvh = kv.shape[1] // (2 * HEAD)
    nh = qd // HEAD
    grp = nh // kvh
    per = 4 if grp % 4 == 0 else 1
    steps = nh // per
    ga = grp // per
    return pl.pallas_call(
        functools.partial(attend_kernel, grp),
        grid_spec=pltpu.PrefetchScalarGridSpec(
            num_scalar_prefetch=1,
            grid=(steps,),
            in_specs=[
                pl.BlockSpec((sd, per * HEAD), lambda i, ci: (0, i)),
                pl.BlockSpec((kv.shape[0], HEAD), lambda i, ci: (0, i // ga)),
                pl.BlockSpec((kv.shape[0], HEAD), lambda i, ci: (0, kvh + i // ga)),
                pl.BlockSpec((sd, HEAD), lambda i, ci: (0, 0)),
                pl.BlockSpec((sd, HEAD), lambda i, ci: (0, 0)),
            ],
            out_specs=pl.BlockSpec((sd, per * HEAD), lambda i, ci: (0, i)),
            scratch_shapes=[pltpu.VMEM((ncp, sd, sd), F32)],
        ),
        out_shape=jax.ShapeDtypeStruct((sd, qd), BF16),
        cost_estimate=pl.CostEstimate(flops=16 * sd * kv.shape[0] * qd, bytes_accessed=8 << 20, transcendentals=0),
        name="attention",
    )(ci, q, kv, kv, c, s)


def combine_kernel(cap, back_ref, gate_ref, ex_ref, zero_ref, u_ref, y_ref, f_ref, h_ref, acc_ref):
    rows = back_ref.shape[0]
    t, nexp = ex_ref.shape
    r = pl.program_id(0) * rows + lax.broadcasted_iota(jnp.int32, (nexp, rows), 1)
    lo = cap * lax.broadcasted_iota(jnp.int32, (nexp, rows), 0)
    own = (r >= lo) & (r < lo + cap)
    spread = jnp.where(own, 1.0, 0.0).astype(BF16)
    slot = jnp.sum(jnp.where(own, (r - lo).astype(F32), 0.0), axis=0, keepdims=True)
    hit = jnp.dot(ex_ref[...], spread, preferred_element_type=F32) == slot
    back = back_ref[...]

    @pl.when(pl.program_id(0) == 0)
    def _():
        acc_ref[...] = zero_ref[:, :1] * u_ref[...].astype(F32)

    tot = None
    for i in range(3):
        w = jnp.dot(gate_ref[i * t:(i + 1) * t, :], spread, preferred_element_type=F32)
        p = jnp.dot(jnp.where(hit, w, 0.0).astype(BF16), back, preferred_element_type=F32)
        tot = p if tot is None else tot + p
    acc_ref[...] += tot

    @pl.when(pl.program_id(0) == pl.num_programs(0) - 1)
    def _():
        h_ref[...] = (y_ref[...].astype(F32) + f_ref[...].astype(F32) + acc_ref[...]).astype(BF16)


def combine(back, gate, ex, zero, u, y, f, cap):
    t, d = u.shape
    nexp = ex.shape[1]
    rows = 16 * cap
    whole = lambda a: pl.BlockSpec(a.shape, lambda i: (0, 0))
    return pl.pallas_call(
        functools.partial(combine_kernel, cap),
        grid=(nexp * cap // rows,),
        out_shape=jax.ShapeDtypeStruct((t, d), BF16),
        in_specs=[pl.BlockSpec((rows, d), lambda i: (i, 0))] + [whole(a) for a in (gate, ex, zero, u, y, f)],
        out_specs=pl.BlockSpec((t, d), lambda i: (0, 0)),
        scratch_shapes=[pltpu.VMEM((t, d), F32)],
        cost_estimate=pl.CostEstimate(flops=6 * nexp * cap * t * d, bytes_accessed=nexp * cap * d * 2, transcendentals=0),
        name="combine",
    )(back, gate, ex, zero, u, y, f)


def solution(mesh):
    ncp = mesh.shape['cp']
    ndev = mesh.shape['b'] * ncp
    tok = P(('dp', 'b'), 'cp', None)
    rep = P()
    exs = P(('b', 'cp'), None, None)
    axes = ('b', 'cp')

    def body(x, ids, g_attn, wq, wk, wv, wo, g_ffn, w1, w3, w2, g_moe, wr, we_g, we_u, we_d):
        bd, sd, d = x.shape
        top = ids.shape[-1]
        x = x.reshape(sd, d)
        ids = ids.reshape(sd, top)
        cap = sd * top // ndev
        ci = lax.axis_index('cp')

        c, s = rope_tables(ci * sd + jnp.arange(sd))
        n, u, kv, gate, zero, ex, ext = front(x, ids, g_attn, g_moe, wk, wv, wr, c, s, ndev)
        kv = lax.all_gather(kv, 'cp', axis=0, tiled=True)
        send = dispatch(ext, u, cap)
        recv = lax.all_to_all(send, axes, 0, 0, tiled=True)

        q = proj(n, wq)
        o = attention(ci.reshape(1), q, kv, c, s, ncp)
        y = (x.astype(F32) + proj(o, wo).astype(F32)).astype(BF16)
        z = rms_norm(y, g_ffn)
        hid = (jax.nn.silu(jnp.dot(z, w1, preferred_element_type=F32)) * jnp.dot(z, w3, preferred_element_type=F32)).astype(BF16)
        f = proj(hid, w2)

        eh = (jax.nn.silu(jnp.dot(recv, we_g[0], preferred_element_type=F32)) * jnp.dot(recv, we_u[0], preferred_element_type=F32)).astype(BF16)
        out = proj(eh, we_d[0])
        back = lax.all_to_all(out, axes, 0, 0, tiled=True)
        h = combine(back, gate, ex, zero, u, y, f, cap)
        return h.reshape(bd, sd, d)

    return jax.shard_map(body, mesh=mesh, in_specs=(tok, tok, rep, rep, rep, rep, rep, rep, rep, rep, rep, rep, rep, exs, exs, exs), out_specs=tok, check_vma=False)
```

```python
import functools

import jax
import jax.numpy as jnp
from jax import lax
from jax.experimental import pallas as pl
from jax.experimental.pallas import tpu as pltpu
from jax.sharding import PartitionSpec as P

HEAD = 128
ROPE = 64
EPS = 1e-6
THETA = 10000.0
RSCALE = 2.5
LOG2E = 1.4426950408889634
F32 = jnp.float32
BF16 = jnp.bfloat16


def rms_norm(x, g):
    xf = x.astype(F32)
    r = lax.rsqrt(jnp.mean(xf * xf, axis=-1, keepdims=True) + EPS)
    return (xf * r * g.astype(F32)).astype(BF16)


def proj(a, wt):
    return jnp.dot(a, wt, preferred_element_type=F32).astype(BF16)


def rope_tables(pos):
    half = ROPE // 2
    freq = THETA ** (-jnp.arange(half, dtype=F32) / half)
    ang = pos.astype(F32)[:, None] * freq[None, :]
    c, s = jnp.cos(ang), jnp.sin(ang)
    rest = jnp.ones((pos.shape[0], HEAD - ROPE), F32)
    return jnp.concatenate([c, c, rest], axis=-1), jnp.concatenate([-s, s, 0.0 * rest], axis=-1)


def rotate(t, c, s):
    half = ROPE // 2
    lane = lax.broadcasted_iota(jnp.int32, t.shape, 1)
    partner = jnp.where(lane < half, pltpu.roll(t, HEAD - half, 1), pltpu.roll(t, half, 1))
    return (t * c + partner * s).astype(BF16)


def vmem(n):
    return [pl.BlockSpec(memory_space=pltpu.VMEM)] * n


def front_kernel(x_ref, ids_ref, ga_ref, gm_ref, wk_ref, wv_ref, wr_ref, c_ref, s_ref, n_ref, u_ref, kv_ref, gate_ref, zero_ref, ex_ref, ext_ref):
    t, d = x_ref.shape
    nexp = ex_ref.shape[1]
    xf = x_ref[...].astype(F32)
    xr = xf * lax.rsqrt(jnp.mean(xf * xf, axis=-1, keepdims=True) + EPS)
    n = (xr * ga_ref[...].astype(F32)).astype(BF16)
    u = (xr * gm_ref[...].astype(F32)).astype(BF16)
    n_ref[...] = n
    u_ref[...] = u
    kd = wk_ref.shape[1]
    k = jnp.dot(n, wk_ref[...], preferred_element_type=F32).astype(BF16).astype(F32)
    for i in range(kd // HEAD):
        kv_ref[:, i * HEAD:(i + 1) * HEAD] = rotate(k[:, i * HEAD:(i + 1) * HEAD], c_ref[...], s_ref[...])
    kv_ref[:, kd:] = jnp.dot(n, wv_ref[...], preferred_element_type=F32).astype(BF16)
    logits = jnp.dot(u, wr_ref[...], preferred_element_type=F32)
    col = lax.broadcasted_iota(jnp.int32, logits.shape, 1)
    ids = ids_ref[...]
    mult = jnp.zeros(logits.shape, F32)
    for j in range(ids.shape[1]):
        mult += (ids[:, j:j + 1] == col).astype(F32)
    has = mult > 0.0
    top = jnp.max(jnp.where(has, logits, -jnp.inf), axis=-1, keepdims=True)
    e = jnp.where(has, mult * jnp.exp(jnp.minimum(logits - top, 0.0)), 0.0)
    gate = RSCALE * e / jnp.sum(e, axis=-1, keepdims=True)
    zero = jnp.sum(jnp.where(col >= nexp, gate, 0.0), axis=-1, keepdims=True)
    zero_ref[...] = jnp.broadcast_to(zero, zero_ref.shape)
    g = gate[:, :nexp]
    for i in range(3):
        part = g.astype(BF16)
        gate_ref[i * t:(i + 1) * t, :] = part
        g = g - part.astype(F32)
    here = has[:, :nexp]
    ti = lax.broadcasted_iota(jnp.int32, (t, t), 0)
    tj = lax.broadcasted_iota(jnp.int32, (t, t), 1)
    before = jnp.where(tj < ti, 1.0, 0.0).astype(BF16)
    rank = jnp.dot(before, jnp.where(here, 1.0, 0.0).astype(BF16), preferred_element_type=F32)
    rank = jnp.where(here, rank, -1.0)
    ex_ref[...] = rank.astype(BF16)
    ext_ref[...] = rank.T.astype(BF16)


def front(x, ids, ga, gm, wk, wv, wr, c, s, nexp):
    t, d = x.shape
    kd = wk.shape[1]
    shapes = [((t, d), BF16), ((t, d), BF16), ((t, 2 * kd), BF16), ((3 * t, nexp), BF16), ((t, HEAD), F32), ((t, nexp), BF16), ((nexp, t), BF16)]
    return pl.pallas_call(
        front_kernel,
        out_shape=[jax.ShapeDtypeStruct(*a) for a in shapes],
        in_specs=vmem(9),
        out_specs=vmem(7),
        cost_estimate=pl.CostEstimate(flops=2 * t * d * (2 * kd + wr.shape[1]), bytes_accessed=8 << 20, transcendentals=0),
        compiler_params=pltpu.CompilerParams(vmem_limit_bytes=48 << 20),
        name="front",
    )(x, ids, ga.reshape(1, d), gm.reshape(1, d), wk, wv, wr, c, s)


def dispatch_kernel(cap, ext_ref, u_ref, o_ref):
    rows = o_ref.shape[0]
    nexp = ext_ref.shape[0]
    r = pl.program_id(0) * rows + lax.broadcasted_iota(jnp.int32, (rows, nexp), 0)
    lo = cap * lax.broadcasted_iota(jnp.int32, (rows, nexp), 1)
    own = (r >= lo) & (r < lo + cap)
    rank = jnp.dot(jnp.where(own, 1.0, 0.0).astype(BF16), ext_ref[...], preferred_element_type=F32)
    slot = jnp.sum(jnp.where(own, (r - lo).astype(F32), 0.0), axis=-1, keepdims=True)
    sel = jnp.where(rank == slot, 1.0, 0.0).astype(BF16)
    o_ref[...] = jnp.dot(sel, u_ref[...], preferred_element_type=F32).astype(BF16)


def dispatch(ext, u, cap):
    nexp, t = ext.shape
    d = u.shape[1]
    rows = 16 * cap
    return pl.pallas_call(
        functools.partial(dispatch_kernel, cap),
        grid=(nexp * cap // rows,),
        out_shape=jax.ShapeDtypeStruct((nexp * cap, d), BF16),
        in_specs=[pl.BlockSpec((nexp, t), lambda i: (0, 0)), pl.BlockSpec((t, d), lambda i: (0, 0))],
        out_specs=pl.BlockSpec((rows, d), lambda i: (i, 0)),
        cost_estimate=pl.CostEstimate(flops=2 * nexp * cap * t * d, bytes_accessed=nexp * cap * d * 2, transcendentals=0),
        name="dispatch",
    )(ext, u)


def attend_kernel(grp, ci_ref, q_ref, k_ref, v_ref, c_ref, s_ref, o_ref, sc_ref):
    sd = q_ref.shape[0]
    ci = ci_ref[0]
    row = lax.broadcasted_iota(jnp.int32, (sd, sd), 0)
    colm = lax.broadcasted_iota(jnp.int32, (sd, sd), 1)
    for h in range(q_ref.shape[1] // HEAD):
        q = rotate(q_ref[:, h * HEAD:(h + 1) * HEAD].astype(F32), c_ref[...], s_ref[...])

        def score(j):
            kb = k_ref[pl.ds(pl.multiple_of(j * sd, sd), sd), :]
            return lax.dot_general(q, kb, (((1,), (1,)), ((), ())), preferred_element_type=F32) * (HEAD ** -0.5 * LOG2E)

        def fold(a, op):
            r = a[:, :HEAD]
            for i in range(1, sd // HEAD):
                r = op(r, a[:, i * HEAD:(i + 1) * HEAD])
            return r

        def first(j, m):
            sc = score(j)
            sc_ref[j] = sc
            return jnp.maximum(m, fold(sc, jnp.maximum))

        last = jnp.where(row >= colm, score(ci), -1e30)
        mx = lax.fori_loop(0, ci, first, fold(last, jnp.maximum))
        mx = jnp.max(mx, axis=-1, keepdims=True)

        def weigh(sc, j, den, acc):
            p = jnp.exp2(sc - mx)
            vb = v_ref[pl.ds(pl.multiple_of(j * sd, sd), sd), :]
            return den + fold(p, jnp.add), acc + jnp.dot(p.astype(BF16), vb, preferred_element_type=F32)

        zero = jnp.zeros((sd, HEAD), F32)
        den, acc = weigh(last, ci, zero, zero)
        den, acc = lax.fori_loop(0, ci, lambda j, st: weigh(sc_ref[j], j, *st), (den, acc))
        o_ref[:, h * HEAD:(h + 1) * HEAD] = (acc / jnp.sum(den, axis=-1, keepdims=True)).astype(BF16)


def attention(ci, q, kv, c, s, ncp):
    sd, qd = q.shape
    kvh = kv.shape[1] // (2 * HEAD)
    nh = qd // HEAD
    grp = nh // kvh
    per = 4 if grp % 4 == 0 else 1
    steps = nh // per
    ga = grp // per
    return pl.pallas_call(
        functools.partial(attend_kernel, grp),
        grid_spec=pltpu.PrefetchScalarGridSpec(
            num_scalar_prefetch=1,
            grid=(steps,),
            in_specs=[
                pl.BlockSpec((sd, per * HEAD), lambda i, ci: (0, i)),
                pl.BlockSpec((kv.shape[0], HEAD), lambda i, ci: (0, i // ga)),
                pl.BlockSpec((kv.shape[0], HEAD), lambda i, ci: (0, kvh + i // ga)),
                pl.BlockSpec((sd, HEAD), lambda i, ci: (0, 0)),
                pl.BlockSpec((sd, HEAD), lambda i, ci: (0, 0)),
            ],
            out_specs=pl.BlockSpec((sd, per * HEAD), lambda i, ci: (0, i)),
            scratch_shapes=[pltpu.VMEM((ncp, sd, sd), F32)],
        ),
        out_shape=jax.ShapeDtypeStruct((sd, qd), BF16),
        cost_estimate=pl.CostEstimate(flops=16 * sd * kv.shape[0] * qd, bytes_accessed=8 << 20, transcendentals=0),
        name="attention",
    )(ci, q, kv, kv, c, s)


def expert_kernel(cap, nb, ncp, ny, recv, wg, wu, wd, gate_ref, ex_ref, zero_ref, u_ref, y_ref, f_ref, h_ref, made, back, ibuf, obuf, bbuf, acc_ref, isem, osem, bsem, ssem, rsem):
    b, c = lax.axis_index('b'), lax.axis_index('cp')
    nz = nb // ny
    me = b * ncp + c
    rows = ncp * cap
    t, nexp = ex_ref.shape

    def shifted(k, sign):
        dy, dz = k % ny, k // ny
        return (b // ny + sign * dz + nz) % nz * ny + (b % ny + sign * dy + ny) % ny

    def block(ref, g):
        return ref.at[pl.ds(pl.multiple_of(g * rows, rows), rows)]

    def chunk(ref, e):
        return ref.at[pl.ds(pl.multiple_of(e * cap, cap), cap)]

    def load(k):
        return pltpu.make_async_copy(block(recv, shifted(k, 1)), ibuf.at[k % 2], isem.at[k % 2])

    def store(k):
        return pltpu.make_async_copy(obuf.at[k % 2], block(made, shifted(k, 1)), osem.at[k % 2])

    def give(g, p):
        return pltpu.make_async_remote_copy(
            src_ref=chunk(made, g * ncp + p), dst_ref=chunk(back, me), send_sem=ssem.at[g * ncp + p], recv_sem=rsem.at[me],
            device_id={'b': g, 'cp': p}, device_id_type=pl.DeviceIdType.MESH)

    def keep():
        return pltpu.make_async_copy(chunk(made, me), chunk(back, me), rsem.at[me])

    def send(k):
        g = shifted(k, 1)

        def one(i, _):
            give(g, (c + i) % ncp).start()
            return 0

        @pl.when(k == 0)
        def _():
            keep().start()

        lax.fori_loop(jnp.where(k == 0, 1, 0), ncp, one, 0)

    load(0).start()

    def work(k, _):
        load(k).wait()

        @pl.when(k + 1 < nb)
        def _():
            load(k + 1).start()

        x = ibuf[k % 2]
        a = jnp.dot(x, wg[...], preferred_element_type=F32)
        hid = (a * (1.0 / (1.0 + jnp.exp(-a))) * jnp.dot(x, wu[...], preferred_element_type=F32)).astype(BF16)

        @pl.when(k > 0)
        def _():
            store(k - 1).wait()
            send(k - 1)

        obuf[k % 2] = jnp.dot(hid, wd[...], preferred_element_type=F32).astype(BF16)
        store(k).start()
        return 0

    lax.fori_loop(0, nb, work, 0)
    store(nb - 1).wait()
    send(nb - 1)

    acc_ref[...] = zero_ref[:, :1] * u_ref[...].astype(F32)

    def fetch(k):
        return pltpu.make_async_copy(block(back, shifted(k, -1)), bbuf.at[k % 2], bsem.at[k % 2])

    def arrive(k):
        g = shifted(k, -1)

        def one(i, _):
            pltpu.make_async_copy(chunk(back, g * ncp + i), chunk(back, g * ncp + i), rsem.at[g * ncp + i]).wait()
            return 0

        lax.fori_loop(0, ncp, one, 0)
        fetch(k).start()

    def add(k, _):
        @pl.when(k < nb)
        def _():
            arrive(k)

        @pl.when(k > 0)
        def _():
            kk = k - 1
            fetch(kk).wait()
            r = shifted(kk, -1) * rows + lax.broadcasted_iota(jnp.int32, (nexp, rows), 1)
            lo = cap * lax.broadcasted_iota(jnp.int32, (nexp, rows), 0)
            own = (r >= lo) & (r < lo + cap)
            spread = jnp.where(own, 1.0, 0.0).astype(BF16)
            slot = jnp.sum(jnp.where(own, (r - lo).astype(F32), 0.0), axis=0, keepdims=True)
            hit = jnp.dot(ex_ref[...], spread, preferred_element_type=F32) == slot
            got = bbuf[kk % 2]
            tot = acc_ref[...]
            for i in range(3):
                w = jnp.dot(gate_ref[i * t:(i + 1) * t, :], spread, preferred_element_type=F32)
                tot += jnp.dot(jnp.where(hit, w, 0.0).astype(BF16), got, preferred_element_type=F32)
            acc_ref[...] = tot

        return 0

    lax.fori_loop(0, nb + 1, add, 0)
    h_ref[...] = (y_ref[...].astype(F32) + f_ref[...].astype(F32) + acc_ref[...]).astype(BF16)

    def drain(k, _):
        g = shifted(k, 1)

        def one(i, _):
            give(g, (c + i) % ncp).wait_send()
            return 0

        lax.fori_loop(jnp.where(k == 0, 1, 0), ncp, one, 0)
        return 0

    lax.fori_loop(0, nb, drain, 0)


def experts(recv, wg, wu, wd, gate, ex, zero, u, y, f, cap, nb, ncp, ny):
    t, d = u.shape
    n, rows = nb * ncp, ncp * cap
    hbm = pl.BlockSpec(memory_space=pl.ANY)
    return pl.pallas_call(
        functools.partial(expert_kernel, cap, nb, ncp, ny),
        out_shape=[jax.ShapeDtypeStruct(a, BF16) for a in ((t, d), recv.shape, recv.shape)],
        in_specs=[hbm] + vmem(9),
        out_specs=vmem(1) + [hbm, hbm],
        scratch_shapes=[
            pltpu.VMEM((2, rows, d), BF16),
            pltpu.VMEM((2, rows, d), BF16),
            pltpu.VMEM((2, rows, d), BF16),
            pltpu.VMEM((t, d), F32),
            pltpu.SemaphoreType.DMA((2,)),
            pltpu.SemaphoreType.DMA((2,)),
            pltpu.SemaphoreType.DMA((2,)),
            pltpu.SemaphoreType.DMA((n,)),
            pltpu.SemaphoreType.DMA((n,)),
        ],
        cost_estimate=pl.CostEstimate(flops=100 << 30, bytes_accessed=32 << 20, transcendentals=0),
        compiler_params=pltpu.CompilerParams(vmem_limit_bytes=56 << 20, has_side_effects=True),
        name="experts",
    )(recv, wg, wu, wd, gate, ex, zero, u, y, f)[0]


def solution(mesh):
    ncp = mesh.shape['cp']
    ndev = mesh.shape['b'] * ncp
    ny = 4 if mesh.shape['b'] % 4 == 0 else 1
    tok = P(('dp', 'b'), 'cp', None)
    rep = P()
    exs = P(('b', 'cp'), None, None)
    axes = ('b', 'cp')

    def body(x, ids, g_attn, wq, wk, wv, wo, g_ffn, w1, w3, w2, g_moe, wr, we_g, we_u, we_d):
        bd, sd, d = x.shape
        top = ids.shape[-1]
        x = x.reshape(sd, d)
        ids = ids.reshape(sd, top)
        cap = sd * top // ndev
        ci = lax.axis_index('cp')

        c, s = rope_tables(ci * sd + jnp.arange(sd))
        n, u, kv, gate, zero, ex, ext = front(x, ids, g_attn, g_moe, wk, wv, wr, c, s, ndev)
        kv = lax.all_gather(kv, 'cp', axis=0, tiled=True)
        send, kv = lax.optimization_barrier((dispatch(ext, u, cap), kv))
        recv = lax.all_to_all(send, axes, 0, 0, tiled=True)

        q = proj(n, wq)
        o = attention(ci.reshape(1), q, kv, c, s, ncp)
        y = (x.astype(F32) + proj(o, wo).astype(F32)).astype(BF16)
        z = rms_norm(y, g_ffn)
        hid = (jax.nn.silu(jnp.dot(z, w1, preferred_element_type=F32)) * jnp.dot(z, w3, preferred_element_type=F32)).astype(BF16)
        f = proj(hid, w2)

        h = experts(recv, we_g[0], we_u[0], we_d[0], gate, ex, zero, u, y, f, cap, ndev // ncp, ncp, ny)
        return h.reshape(bd, sd, d)

    return jax.shard_map(body, mesh=mesh, in_specs=(tok, tok, rep, rep, rep, rep, rep, rep, rep, rep, rep, rep, rep, exs, exs, exs), out_specs=tok, check_vma=False)
```

```python
import functools

import jax
import jax.numpy as jnp
from jax import lax
from jax.experimental import pallas as pl
from jax.experimental.pallas import tpu as pltpu
from jax.sharding import PartitionSpec as P

HEAD = 128
ROPE = 64
EPS = 1e-6
THETA = 10000.0
RSCALE = 2.5
PARTS = 2
LOG2E = 1.4426950408889634
F32 = jnp.float32
BF16 = jnp.bfloat16


def rms_norm(x, g):
    xf = x.astype(F32)
    r = lax.rsqrt(jnp.mean(xf * xf, axis=-1, keepdims=True) + EPS)
    return (xf * r * g.astype(F32)).astype(BF16)


def proj(a, wt):
    return jnp.dot(a, wt, preferred_element_type=F32).astype(BF16)


def rope_tables(pos):
    half = ROPE // 2
    freq = THETA ** (-jnp.arange(half, dtype=F32) / half)
    ang = pos.astype(F32)[:, None] * freq[None, :]
    c, s = jnp.cos(ang), jnp.sin(ang)
    rest = jnp.ones((pos.shape[0], HEAD - ROPE), F32)
    return jnp.concatenate([c, c, rest], axis=-1), jnp.concatenate([-s, s, 0.0 * rest], axis=-1)


def rotate(t, c, s):
    half = ROPE // 2
    lane = lax.broadcasted_iota(jnp.int32, t.shape, 1)
    partner = jnp.where(lane < half, pltpu.roll(t, HEAD - half, 1), pltpu.roll(t, half, 1))
    return (t * c + partner * s).astype(BF16)


def vmem(n):
    return [pl.BlockSpec(memory_space=pltpu.VMEM)] * n


def front_kernel(x_ref, ids_ref, ga_ref, gm_ref, wk_ref, wv_ref, wr_ref, c_ref, s_ref, n_ref, u_ref, kv_ref, gate_ref, zero_ref, ex_ref, ext_ref):
    t, d = x_ref.shape
    nexp = ex_ref.shape[1]
    xf = x_ref[...].astype(F32)
    xr = xf * lax.rsqrt(jnp.mean(xf * xf, axis=-1, keepdims=True) + EPS)
    n = (xr * ga_ref[...].astype(F32)).astype(BF16)
    u = (xr * gm_ref[...].astype(F32)).astype(BF16)
    n_ref[...] = n
    u_ref[...] = u
    kd = wk_ref.shape[1]
    k = jnp.dot(n, wk_ref[...], preferred_element_type=F32).astype(BF16).astype(F32)
    for i in range(kd // HEAD):
        kv_ref[:, i * HEAD:(i + 1) * HEAD] = rotate(k[:, i * HEAD:(i + 1) * HEAD], c_ref[...], s_ref[...])
    kv_ref[:, kd:] = jnp.dot(n, wv_ref[...], preferred_element_type=F32).astype(BF16)
    logits = jnp.dot(u, wr_ref[...], preferred_element_type=F32)
    col = lax.broadcasted_iota(jnp.int32, logits.shape, 1)
    ids = ids_ref[...]
    mult = jnp.zeros(logits.shape, F32)
    for j in range(ids.shape[1]):
        mult += (ids[:, j:j + 1] == col).astype(F32)
    has = mult > 0.0
    top = jnp.max(jnp.where(has, logits, -jnp.inf), axis=-1, keepdims=True)
    e = jnp.where(has, mult * jnp.exp(jnp.minimum(logits - top, 0.0)), 0.0)
    gate = RSCALE * e / jnp.sum(e, axis=-1, keepdims=True)
    zero = jnp.sum(jnp.where(col >= nexp, gate, 0.0), axis=-1, keepdims=True)
    zero_ref[...] = jnp.broadcast_to(zero, zero_ref.shape)
    g = gate[:, :nexp]
    for i in range(3):
        part = g.astype(BF16)
        gate_ref[i * t:(i + 1) * t, :] = part
        g = g - part.astype(F32)
    here = has[:, :nexp]
    ti = lax.broadcasted_iota(jnp.int32, (t, t), 0)
    tj = lax.broadcasted_iota(jnp.int32, (t, t), 1)
    before = jnp.where(tj < ti, 1.0, 0.0).astype(BF16)
    rank = jnp.dot(before, jnp.where(here, 1.0, 0.0).astype(BF16), preferred_element_type=F32)
    rank = jnp.where(here, rank, -1.0)
    ex_ref[...] = rank.astype(BF16)
    ext_ref[...] = rank.T.astype(BF16)


def front(x, ids, ga, gm, wk, wv, wr, c, s, nexp):
    t, d = x.shape
    kd = wk.shape[1]
    shapes = [((t, d), BF16), ((t, d), BF16), ((t, 2 * kd), BF16), ((3 * t, nexp), BF16), ((t, HEAD), F32), ((t, nexp), BF16), ((nexp, t), BF16)]
    return pl.pallas_call(
        front_kernel,
        out_shape=[jax.ShapeDtypeStruct(*a) for a in shapes],
        in_specs=vmem(9),
        out_specs=vmem(7),
        cost_estimate=pl.CostEstimate(flops=2 * t * d * (2 * kd + wr.shape[1]), bytes_accessed=8 << 20, transcendentals=0),
        compiler_params=pltpu.CompilerParams(vmem_limit_bytes=48 << 20),
        name="front",
    )(x, ids, ga.reshape(1, d), gm.reshape(1, d), wk, wv, wr, c, s)


def dispatch_kernel(cap, ext_ref, u_ref, o_ref):
    rows = o_ref.shape[0]
    nexp = ext_ref.shape[0]
    r = pl.program_id(0) * rows + lax.broadcasted_iota(jnp.int32, (rows, nexp), 0)
    lo = cap * lax.broadcasted_iota(jnp.int32, (rows, nexp), 1)
    own = (r >= lo) & (r < lo + cap)
    rank = jnp.dot(jnp.where(own, 1.0, 0.0).astype(BF16), ext_ref[...], preferred_element_type=F32)
    slot = jnp.sum(jnp.where(own, (r - lo).astype(F32), 0.0), axis=-1, keepdims=True)
    sel = jnp.where(rank == slot, 1.0, 0.0).astype(BF16)
    o_ref[...] = jnp.dot(sel, u_ref[...], preferred_element_type=F32).astype(BF16)


def dispatch(ext, u, cap):
    nexp, t = ext.shape
    d = u.shape[1]
    rows = 16 * cap
    return pl.pallas_call(
        functools.partial(dispatch_kernel, cap),
        grid=(nexp * cap // rows,),
        out_shape=jax.ShapeDtypeStruct((nexp * cap, d), BF16),
        in_specs=[pl.BlockSpec((nexp, t), lambda i: (0, 0)), pl.BlockSpec((t, d), lambda i: (0, 0))],
        out_specs=pl.BlockSpec((rows, d), lambda i: (i, 0)),
        cost_estimate=pl.CostEstimate(flops=2 * nexp * cap * t * d, bytes_accessed=nexp * cap * d * 2, transcendentals=0),
        name="dispatch",
    )(ext, u)


def attend_kernel(per, ci_ref, q_ref, k_ref, v_ref, c_ref, s_ref, o_ref, q_all, sc_ref, mx_ref, den_ref, acc_ref):
    sd = q_ref.shape[0]
    ci = ci_ref[0]
    for h in range(per):
        q_all[h * sd:(h + 1) * sd, :] = rotate(q_ref[:, h * HEAD:(h + 1) * HEAD].astype(F32), c_ref[...], s_ref[...])

    def fold(a, op):
        r = a[:, :HEAD]
        for i in range(1, sd // HEAD):
            r = op(r, a[:, i * HEAD:(i + 1) * HEAD])
        return r

    def score(j):
        kb = k_ref[pl.ds(pl.multiple_of(j * sd, sd), sd), :]
        return lax.dot_general(q_all[...], kb, (((1,), (1,)), ((), ())), preferred_element_type=F32) * (HEAD ** -0.5 * LOG2E)

    row = lax.broadcasted_iota(jnp.int32, (per * sd, sd), 0) % sd
    last = jnp.where(row >= lax.broadcasted_iota(jnp.int32, (per * sd, sd), 1), score(ci), -1e30)
    sc_ref[ci] = last
    mx_ref[...] = fold(last, jnp.maximum)

    def first(j, _):
        sc = score(j)
        sc_ref[j] = sc
        mx_ref[...] = jnp.maximum(mx_ref[...], fold(sc, jnp.maximum))
        return 0

    lax.fori_loop(0, ci, first, 0)
    mx_ref[...] = jnp.broadcast_to(jnp.max(mx_ref[...], axis=-1, keepdims=True), mx_ref.shape)
    den_ref[...] = jnp.zeros_like(den_ref)
    acc_ref[...] = jnp.zeros_like(acc_ref)

    def second(j, _):
        mx = mx_ref[...]
        p = [jnp.exp2(sc_ref[j, :, i * HEAD:(i + 1) * HEAD] - mx) for i in range(sd // HEAD)]
        den_ref[...] += functools.reduce(jnp.add, p)
        vb = v_ref[pl.ds(pl.multiple_of(j * sd, sd), sd), :]
        acc_ref[...] += jnp.dot(jnp.concatenate([a.astype(BF16) for a in p], axis=-1), vb, preferred_element_type=F32)
        return 0

    lax.fori_loop(0, ci + 1, second, 0)
    o = (acc_ref[...] / jnp.sum(den_ref[...], axis=-1, keepdims=True)).astype(BF16)
    for h in range(per):
        o_ref[:, h * HEAD:(h + 1) * HEAD] = o[h * sd:(h + 1) * sd, :]


def attention(ci, q, kv, c, s, ncp):
    sd, qd = q.shape
    kvh = kv.shape[1] // (2 * HEAD)
    nh = qd // HEAD
    grp = nh // kvh
    per = 4 if grp % 4 == 0 else 1
    steps = nh // per
    ga = grp // per
    return pl.pallas_call(
        functools.partial(attend_kernel, per),
        grid_spec=pltpu.PrefetchScalarGridSpec(
            num_scalar_prefetch=1,
            grid=(steps,),
            in_specs=[
                pl.BlockSpec((sd, per * HEAD), lambda i, ci: (0, i)),
                pl.BlockSpec((kv.shape[0], HEAD), lambda i, ci: (0, i // ga)),
                pl.BlockSpec((kv.shape[0], HEAD), lambda i, ci: (0, kvh + i // ga)),
                pl.BlockSpec((sd, HEAD), lambda i, ci: (0, 0)),
                pl.BlockSpec((sd, HEAD), lambda i, ci: (0, 0)),
            ],
            out_specs=pl.BlockSpec((sd, per * HEAD), lambda i, ci: (0, i)),
            scratch_shapes=[pltpu.VMEM((per * sd, HEAD), BF16), pltpu.VMEM((ncp, per * sd, sd), F32)] + [pltpu.VMEM((per * sd, HEAD), F32)] * 3,
        ),
        out_shape=jax.ShapeDtypeStruct((sd, qd), BF16),
        cost_estimate=pl.CostEstimate(flops=16 * sd * kv.shape[0] * qd, bytes_accessed=8 << 20, transcendentals=0),
        name="attention",
    )(ci, q, kv, kv, c, s)


def hidden_kernel(x_ref, g_ref, w_ref, o_ref):
    x = x_ref[...]
    a = jnp.dot(x, g_ref[...], preferred_element_type=F32)
    o_ref[...] = (a * (1.0 / (1.0 + jnp.exp(-a))) * jnp.dot(x, w_ref[...], preferred_element_type=F32)).astype(BF16)


def hidden(x, wg, wu, rows):
    n, d = x.shape
    ff = wg.shape[1]
    return pl.pallas_call(
        hidden_kernel,
        grid=(n // rows,),
        out_shape=jax.ShapeDtypeStruct((n, ff), BF16),
        in_specs=[pl.BlockSpec((rows, d), lambda i: (i, 0)), pl.BlockSpec((d, ff), lambda i: (0, 0)), pl.BlockSpec((d, ff), lambda i: (0, 0))],
        out_specs=pl.BlockSpec((rows, ff), lambda i: (i, 0)),
        cost_estimate=pl.CostEstimate(flops=4 * n * d * ff, bytes_accessed=n * d * 2, transcendentals=0),
        compiler_params=pltpu.CompilerParams(vmem_limit_bytes=48 << 20),
        name="hidden",
    )(x, wg, wu)


def combine_kernel(cap, back_ref, gate_ref, ex_ref, zero_ref, u_ref, y_ref, f_ref, *rest):
    h_ref, acc_ref = rest[-2:]
    rows = back_ref.shape[0]
    t, nexp = ex_ref.shape
    r = pl.program_id(0) * rows + lax.broadcasted_iota(jnp.int32, (nexp, rows), 1)
    lo = cap * lax.broadcasted_iota(jnp.int32, (nexp, rows), 0)
    own = (r >= lo) & (r < lo + cap)
    spread = jnp.where(own, 1.0, 0.0).astype(BF16)
    slot = jnp.sum(jnp.where(own, (r - lo).astype(F32), 0.0), axis=0, keepdims=True)
    hit = jnp.dot(ex_ref[...], spread, preferred_element_type=F32) == slot
    back = back_ref[...]

    @pl.when(pl.program_id(0) == 0)
    def _():
        acc_ref[...] = zero_ref[:, :1] * u_ref[...].astype(F32)

    tot = None
    for i in range(3):
        w = jnp.dot(gate_ref[i * t:(i + 1) * t, :], spread, preferred_element_type=F32)
        p = jnp.dot(jnp.where(hit, w, 0.0).astype(BF16), back, preferred_element_type=F32)
        tot = p if tot is None else tot + p
    acc_ref[...] += tot

    @pl.when(pl.program_id(0) == pl.num_programs(0) - 1)
    def _():
        h_ref[...] = (y_ref[...].astype(F32) + f_ref[...].astype(F32) + acc_ref[...]).astype(BF16)


def combine(back, gate, ex, zero, u, y, f, cap, part, prior):
    t, d = u.shape
    nexp = ex.shape[1]
    rows = 16 * cap
    cols = back.shape[1]
    whole = lambda a: pl.BlockSpec(a.shape, lambda i: (0, 0))
    mine = pl.BlockSpec((t, cols), lambda i: (0, part))
    return pl.pallas_call(
        functools.partial(combine_kernel, cap),
        grid=(nexp * cap // rows,),
        out_shape=jax.ShapeDtypeStruct((t, d), BF16),
        in_specs=[pl.BlockSpec((rows, cols), lambda i: (i, 0))] + [whole(a) for a in (gate, ex, zero)] + [mine] * 3 + [pl.BlockSpec(memory_space=pl.ANY)] * len(prior),
        out_specs=mine,
        scratch_shapes=[pltpu.VMEM((t, cols), F32)],
        input_output_aliases={7: 0} if prior else {},
        cost_estimate=pl.CostEstimate(flops=6 * nexp * cap * t * cols, bytes_accessed=nexp * cap * cols * 2, transcendentals=0),
        name="combine",
    )(back, gate, ex, zero, u, y, f, *prior)


def solution(mesh):
    ncp = mesh.shape['cp']
    ndev = mesh.shape['b'] * ncp
    tok = P(('dp', 'b'), 'cp', None)
    rep = P()
    exs = P(('b', 'cp'), None, None)
    axes = ('b', 'cp')

    def body(x, ids, g_attn, wq, wk, wv, wo, g_ffn, w1, w3, w2, g_moe, wr, we_g, we_u, we_d):
        bd, sd, d = x.shape
        top = ids.shape[-1]
        x = x.reshape(sd, d)
        ids = ids.reshape(sd, top)
        cap = sd * top // ndev
        ci = lax.axis_index('cp')

        c, s = rope_tables(ci * sd + jnp.arange(sd))
        n, u, kv, gate, zero, ex, ext = front(x, ids, g_attn, g_moe, wk, wv, wr, c, s, ndev)
        send = dispatch(ext, u, cap)
        recv = lax.all_to_all(send, axes, 0, 0, tiled=True)
        q = proj(n, wq)
        recv, kv = lax.optimization_barrier((recv, kv))
        kv = lax.all_gather(kv, 'cp', axis=0, tiled=True)

        hid = hidden(recv, we_g[0], we_u[0], 16 * cap)
        wd = we_d[0]
        cols = d // PARTS
        back = []
        for i in range(PARTS):
            out = proj(hid, wd[:, i * cols:(i + 1) * cols])
            back.append(lax.all_to_all(out, axes, 0, 0, tiled=True))

        o = attention(ci.reshape(1), q, kv, c, s, ncp)
        y = (x.astype(F32) + proj(o, wo).astype(F32)).astype(BF16)
        z = rms_norm(y, g_ffn)
        wide = (jax.nn.silu(jnp.dot(z, w1, preferred_element_type=F32)) * jnp.dot(z, w3, preferred_element_type=F32)).astype(BF16)
        f = proj(wide, w2)

        h = ()
        for i in range(PARTS):
            h = (combine(back[i], gate, ex, zero, u, y, f, cap, i, h),)
        h = h[0]
        return h.reshape(bd, sd, d)

    return jax.shard_map(body, mesh=mesh, in_specs=(tok, tok, rep, rep, rep, rep, rep, rep, rep, rep, rep, rep, rep, exs, exs, exs), out_specs=tok, check_vma=False)
```

```python
import functools

import jax
import jax.numpy as jnp
from jax import lax
from jax.experimental import pallas as pl
from jax.experimental.pallas import tpu as pltpu
from jax.sharding import PartitionSpec as P

HEAD = 128
ROPE = 64
EPS = 1e-6
THETA = 10000.0
RSCALE = 2.5
PARTS = 2
LOG2E = 1.4426950408889634
F32 = jnp.float32
BF16 = jnp.bfloat16


def rms_norm(x, g):
    xf = x.astype(F32)
    r = lax.rsqrt(jnp.mean(xf * xf, axis=-1, keepdims=True) + EPS)
    return (xf * r * g.astype(F32)).astype(BF16)


def proj(a, wt):
    return jnp.dot(a, wt, preferred_element_type=F32).astype(BF16)


def rope_tables(pos):
    half = ROPE // 2
    freq = THETA ** (-jnp.arange(half, dtype=F32) / half)
    ang = pos.astype(F32)[:, None] * freq[None, :]
    c, s = jnp.cos(ang), jnp.sin(ang)
    rest = jnp.ones((pos.shape[0], HEAD - ROPE), F32)
    return jnp.concatenate([c, c, rest], axis=-1), jnp.concatenate([-s, s, 0.0 * rest], axis=-1)


def rotate(t, c, s):
    half = ROPE // 2
    lane = lax.broadcasted_iota(jnp.int32, t.shape, 1)
    partner = jnp.where(lane < half, pltpu.roll(t, HEAD - half, 1), pltpu.roll(t, half, 1))
    return (t * c + partner * s).astype(BF16)


def vmem(n):
    return [pl.BlockSpec(memory_space=pltpu.VMEM)] * n


def front_kernel(x_ref, ids_ref, ga_ref, gm_ref, wk_ref, wv_ref, wr_ref, c_ref, s_ref, n_ref, u_ref, kv_ref, gate_ref, zero_ref, ex_ref, ext_ref):
    t, d = x_ref.shape
    nexp = ex_ref.shape[1]
    xf = x_ref[...].astype(F32)
    xr = xf * lax.rsqrt(jnp.mean(xf * xf, axis=-1, keepdims=True) + EPS)
    n = (xr * ga_ref[...].astype(F32)).astype(BF16)
    u = (xr * gm_ref[...].astype(F32)).astype(BF16)
    n_ref[...] = n
    u_ref[...] = u
    kd = wk_ref.shape[1]
    k = jnp.dot(n, wk_ref[...], preferred_element_type=F32).astype(BF16).astype(F32)
    for i in range(kd // HEAD):
        kv_ref[:, i * HEAD:(i + 1) * HEAD] = rotate(k[:, i * HEAD:(i + 1) * HEAD], c_ref[...], s_ref[...])
    kv_ref[:, kd:] = jnp.dot(n, wv_ref[...], preferred_element_type=F32).astype(BF16)
    logits = jnp.dot(u, wr_ref[...], preferred_element_type=F32)
    col = lax.broadcasted_iota(jnp.int32, logits.shape, 1)
    ids = ids_ref[...]
    mult = jnp.zeros(logits.shape, F32)
    for j in range(ids.shape[1]):
        mult += (ids[:, j:j + 1] == col).astype(F32)
    has = mult > 0.0
    top = jnp.max(jnp.where(has, logits, -jnp.inf), axis=-1, keepdims=True)
    e = jnp.where(has, mult * jnp.exp(jnp.minimum(logits - top, 0.0)), 0.0)
    gate = RSCALE * e / jnp.sum(e, axis=-1, keepdims=True)
    zero = jnp.sum(jnp.where(col >= nexp, gate, 0.0), axis=-1, keepdims=True)
    zero_ref[...] = jnp.broadcast_to(zero, zero_ref.shape)
    g = gate[:, :nexp]
    for i in range(3):
        part = g.astype(BF16)
        gate_ref[i * t:(i + 1) * t, :] = part
        g = g - part.astype(F32)
    here = has[:, :nexp]
    ti = lax.broadcasted_iota(jnp.int32, (t, t), 0)
    tj = lax.broadcasted_iota(jnp.int32, (t, t), 1)
    before = jnp.where(tj < ti, 1.0, 0.0).astype(BF16)
    rank = jnp.dot(before, jnp.where(here, 1.0, 0.0).astype(BF16), preferred_element_type=F32)
    rank = jnp.where(here, rank, -1.0)
    ex_ref[...] = rank.astype(BF16)
    ext_ref[...] = rank.T.astype(BF16)


def front_dispatch_kernel(cap, *refs):
    *first, o_ref, ext_ref = refs

    @pl.when(pl.program_id(0) == 0)
    def _():
        front_kernel(*first, ext_ref)

    u_ref = first[10]
    rows = o_ref.shape[0]
    nexp = ext_ref.shape[0]
    r = pl.program_id(0) * rows + lax.broadcasted_iota(jnp.int32, (rows, nexp), 0)
    lo = cap * lax.broadcasted_iota(jnp.int32, (rows, nexp), 1)
    own = (r >= lo) & (r < lo + cap)
    rank = jnp.dot(jnp.where(own, 1.0, 0.0).astype(BF16), ext_ref[...], preferred_element_type=F32)
    slot = jnp.sum(jnp.where(own, (r - lo).astype(F32), 0.0), axis=-1, keepdims=True)
    sel = jnp.where(rank == slot, 1.0, 0.0).astype(BF16)
    o_ref[...] = jnp.dot(sel, u_ref[...], preferred_element_type=F32).astype(BF16)


def front(x, ids, ga, gm, wk, wv, wr, c, s, nexp, cap):
    t, d = x.shape
    kd = wk.shape[1]
    rows = 16 * cap
    shapes = [((t, d), BF16), ((t, d), BF16), ((t, 2 * kd), BF16), ((3 * t, nexp), BF16), ((t, HEAD), F32), ((t, nexp), BF16)]
    args = (x, ids, ga.reshape(1, d), gm.reshape(1, d), wk, wv, wr, c, s)
    whole = lambda sh: pl.BlockSpec(sh, lambda i: (0, 0))
    return pl.pallas_call(
        functools.partial(front_dispatch_kernel, cap),
        grid=(nexp * cap // rows,),
        out_shape=[jax.ShapeDtypeStruct(*a) for a in shapes] + [jax.ShapeDtypeStruct((nexp * cap, d), BF16)],
        in_specs=[whole(a.shape) for a in args],
        out_specs=[whole(sh) for sh, _ in shapes] + [pl.BlockSpec((rows, d), lambda i: (i, 0))],
        scratch_shapes=[pltpu.VMEM((nexp, t), BF16)],
        cost_estimate=pl.CostEstimate(flops=2 * t * d * (2 * kd + wr.shape[1] + nexp * cap), bytes_accessed=20 << 20, transcendentals=0),
        compiler_params=pltpu.CompilerParams(vmem_limit_bytes=56 << 20),
        name="front",
    )(*args)


def attend_kernel(per, ci_ref, q_ref, k_ref, v_ref, c_ref, s_ref, o_ref, q_all, sc_ref, mx_ref, den_ref, acc_ref):
    sd = q_ref.shape[0]
    ci = ci_ref[0]
    for h in range(per):
        q_all[h * sd:(h + 1) * sd, :] = rotate(q_ref[:, h * HEAD:(h + 1) * HEAD].astype(F32), c_ref[...], s_ref[...])

    def fold(a, op):
        r = a[:, :HEAD]
        for i in range(1, sd // HEAD):
            r = op(r, a[:, i * HEAD:(i + 1) * HEAD])
        return r

    def score(j):
        kb = k_ref[pl.ds(pl.multiple_of(j * sd, sd), sd), :]
        return lax.dot_general(q_all[...], kb, (((1,), (1,)), ((), ())), preferred_element_type=F32) * (HEAD ** -0.5 * LOG2E)

    row = lax.broadcasted_iota(jnp.int32, (per * sd, sd), 0) % sd
    last = jnp.where(row >= lax.broadcasted_iota(jnp.int32, (per * sd, sd), 1), score(ci), -1e30)
    sc_ref[ci] = last
    mx_ref[...] = fold(last, jnp.maximum)

    def first(j, _):
        sc = score(j)
        sc_ref[j] = sc
        mx_ref[...] = jnp.maximum(mx_ref[...], fold(sc, jnp.maximum))
        return 0

    lax.fori_loop(0, ci, first, 0)
    mx_ref[...] = jnp.broadcast_to(jnp.max(mx_ref[...], axis=-1, keepdims=True), mx_ref.shape)
    den_ref[...] = jnp.zeros_like(den_ref)
    acc_ref[...] = jnp.zeros_like(acc_ref)

    def second(j, _):
        mx = mx_ref[...]
        p = [jnp.exp2(sc_ref[j, :, i * HEAD:(i + 1) * HEAD] - mx) for i in range(sd // HEAD)]
        den_ref[...] += functools.reduce(jnp.add, p)
        vb = v_ref[pl.ds(pl.multiple_of(j * sd, sd), sd), :]
        acc_ref[...] += jnp.dot(jnp.concatenate([a.astype(BF16) for a in p], axis=-1), vb, preferred_element_type=F32)
        return 0

    lax.fori_loop(0, ci + 1, second, 0)
    o = (acc_ref[...] / jnp.sum(den_ref[...], axis=-1, keepdims=True)).astype(BF16)
    for h in range(per):
        o_ref[:, h * HEAD:(h + 1) * HEAD] = o[h * sd:(h + 1) * sd, :]


def attention(ci, q, kv, c, s, ncp):
    sd, qd = q.shape
    kvh = kv.shape[1] // (2 * HEAD)
    nh = qd // HEAD
    grp = nh // kvh
    per = 4 if grp % 4 == 0 else 1
    steps = nh // per
    ga = grp // per
    return pl.pallas_call(
        functools.partial(attend_kernel, per),
        grid_spec=pltpu.PrefetchScalarGridSpec(
            num_scalar_prefetch=1,
            grid=(steps,),
            in_specs=[
                pl.BlockSpec((sd, per * HEAD), lambda i, ci: (0, i)),
                pl.BlockSpec((kv.shape[0], HEAD), lambda i, ci: (0, i // ga)),
                pl.BlockSpec((kv.shape[0], HEAD), lambda i, ci: (0, kvh + i // ga)),
                pl.BlockSpec((sd, HEAD), lambda i, ci: (0, 0)),
                pl.BlockSpec((sd, HEAD), lambda i, ci: (0, 0)),
            ],
            out_specs=pl.BlockSpec((sd, per * HEAD), lambda i, ci: (0, i)),
            scratch_shapes=[pltpu.VMEM((per * sd, HEAD), BF16), pltpu.VMEM((ncp, per * sd, sd), F32)] + [pltpu.VMEM((per * sd, HEAD), F32)] * 3,
        ),
        out_shape=jax.ShapeDtypeStruct((sd, qd), BF16),
        cost_estimate=pl.CostEstimate(flops=16 * sd * kv.shape[0] * qd, bytes_accessed=8 << 20, transcendentals=0),
        name="attention",
    )(ci, q, kv, kv, c, s)


def hidden_kernel(ncp, x_ref, g_ref, w_ref, kv_ref, o_ref, all_ref, send_sem, recv_sem):
    c = lax.axis_index('cp')
    rows = kv_ref.shape[0]

    def place(p):
        return all_ref.at[pl.ds(pl.multiple_of(p * rows, rows), rows)]

    def give(p):
        return pltpu.make_async_remote_copy(
            src_ref=kv_ref, dst_ref=place(c), send_sem=send_sem.at[p], recv_sem=recv_sem.at[c],
            device_id={'cp': p}, device_id_type=pl.DeviceIdType.MESH)

    def keep():
        return pltpu.make_async_copy(kv_ref, place(c), recv_sem.at[c])

    def loop(lo, hi, f):
        lax.fori_loop(lo, hi, lambda p, _: (f(p), 0)[1], 0)

    @pl.when(pl.program_id(0) == 0)
    def _():
        loop(c + 1, ncp, lambda p: give(p).start())
        keep().start()

    x = x_ref[...]
    a = jnp.dot(x, g_ref[...], preferred_element_type=F32)
    o_ref[...] = (a * (1.0 / (1.0 + jnp.exp(-a))) * jnp.dot(x, w_ref[...], preferred_element_type=F32)).astype(BF16)

    @pl.when(pl.program_id(0) == pl.num_programs(0) - 1)
    def _():
        loop(0, c + 1, lambda p: pltpu.make_async_copy(place(p), place(p), recv_sem.at[p]).wait())
        loop(c + 1, ncp, lambda p: give(p).wait_send())


def hidden(x, wg, wu, kv, rows, ncp):
    n, d = x.shape
    ff = wg.shape[1]
    hbm = pl.BlockSpec(memory_space=pl.ANY)
    return pl.pallas_call(
        functools.partial(hidden_kernel, ncp),
        grid=(n // rows,),
        out_shape=[jax.ShapeDtypeStruct((n, ff), BF16), jax.ShapeDtypeStruct((ncp * kv.shape[0], kv.shape[1]), BF16)],
        in_specs=[pl.BlockSpec((rows, d), lambda i: (i, 0)), pl.BlockSpec((d, ff), lambda i: (0, 0)), pl.BlockSpec((d, ff), lambda i: (0, 0)), hbm],
        out_specs=[pl.BlockSpec((rows, ff), lambda i: (i, 0)), hbm],
        scratch_shapes=[pltpu.SemaphoreType.DMA((ncp,)), pltpu.SemaphoreType.DMA((ncp,))],
        cost_estimate=pl.CostEstimate(flops=4 * n * d * ff, bytes_accessed=n * d * 2, transcendentals=0),
        compiler_params=pltpu.CompilerParams(vmem_limit_bytes=48 << 20, has_side_effects=True),
        name="hidden",
    )(x, wg, wu, kv)


def weigh_kernel(cap, gate_ref, ex_ref, w_ref):
    rows = w_ref.shape[1]
    t, nexp = ex_ref.shape
    r = pl.program_id(0) * rows + lax.broadcasted_iota(jnp.int32, (nexp, rows), 1)
    lo = cap * lax.broadcasted_iota(jnp.int32, (nexp, rows), 0)
    own = (r >= lo) & (r < lo + cap)
    spread = jnp.where(own, 1.0, 0.0).astype(BF16)
    slot = jnp.sum(jnp.where(own, (r - lo).astype(F32), 0.0), axis=0, keepdims=True)
    hit = jnp.dot(ex_ref[...], spread, preferred_element_type=F32) == slot
    for i in range(3):
        w = jnp.dot(gate_ref[i * t:(i + 1) * t, :], spread, preferred_element_type=F32)
        w_ref[i * t:(i + 1) * t, :] = jnp.where(hit, w, 0.0).astype(BF16)


def weigh(gate, ex, cap):
    t3, nexp = gate.shape
    rows = 16 * cap
    whole = lambda a: pl.BlockSpec(a.shape, lambda i: (0, 0))
    return pl.pallas_call(
        functools.partial(weigh_kernel, cap),
        grid=(nexp * cap // rows,),
        out_shape=jax.ShapeDtypeStruct((t3, nexp * cap), BF16),
        in_specs=[whole(gate), whole(ex)],
        out_specs=pl.BlockSpec((t3, rows), lambda i: (0, i)),
        cost_estimate=pl.CostEstimate(flops=3 * t3 * nexp * nexp * cap, bytes_accessed=t3 * nexp * cap * 2, transcendentals=0),
        name="weigh",
    )(gate, ex)


def combine_kernel(back_ref, w_ref, zero_ref, u_ref, y_ref, f_ref, *rest):
    h_ref, acc_ref = rest[-2:]
    t = u_ref.shape[0]

    @pl.when(pl.program_id(0) == 0)
    def _():
        acc_ref[...] = zero_ref[:, :1] * u_ref[...].astype(F32)

    p = jnp.dot(w_ref[...], back_ref[...], preferred_element_type=F32)
    acc_ref[...] += p[:t] + p[t:2 * t] + p[2 * t:]

    @pl.when(pl.program_id(0) == pl.num_programs(0) - 1)
    def _():
        h_ref[...] = (y_ref[...].astype(F32) + f_ref[...].astype(F32) + acc_ref[...]).astype(BF16)


def combine(back, w, zero, u, y, f, rows, part, prior):
    t, d = u.shape
    n, cols = back.shape
    whole = lambda a: pl.BlockSpec(a.shape, lambda i: (0, 0))
    mine = pl.BlockSpec((t, cols), lambda i: (0, part))
    return pl.pallas_call(
        combine_kernel,
        grid=(n // rows,),
        out_shape=jax.ShapeDtypeStruct((t, d), BF16),
        in_specs=[pl.BlockSpec((rows, cols), lambda i: (i, 0))] + [pl.BlockSpec((3 * t, rows), lambda i: (0, i)), whole(zero)] + [mine] * 3 + [pl.BlockSpec(memory_space=pl.ANY)] * len(prior),
        out_specs=mine,
        scratch_shapes=[pltpu.VMEM((t, cols), F32)],
        input_output_aliases={6: 0} if prior else {},
        cost_estimate=pl.CostEstimate(flops=6 * n * t * cols, bytes_accessed=n * (cols + 3 * t) * 2, transcendentals=0),
        name="combine",
    )(back, w, zero, u, y, f, *prior)


def solution(mesh):
    ncp = mesh.shape['cp']
    ndev = mesh.shape['b'] * ncp
    tok = P(('dp', 'b'), 'cp', None)
    rep = P()
    exs = P(('b', 'cp'), None, None)
    axes = ('b', 'cp')

    def body(x, ids, g_attn, wq, wk, wv, wo, g_ffn, w1, w3, w2, g_moe, wr, we_g, we_u, we_d):
        bd, sd, d = x.shape
        top = ids.shape[-1]
        x = x.reshape(sd, d)
        ids = ids.reshape(sd, top)
        cap = sd * top // ndev
        ci = lax.axis_index('cp')

        c, s = rope_tables(ci * sd + jnp.arange(sd))
        n, u, kv, gate, zero, ex, send = front(x, ids, g_attn, g_moe, wk, wv, wr, c, s, ndev, cap)
        recv = lax.all_to_all(send, axes, 0, 0, tiled=True)
        q = proj(n, wq)

        hid, kv = hidden(recv, we_g[0], we_u[0], kv, 16 * cap, ncp)
        wd = we_d[0]
        cols = d // PARTS
        back = []
        for i in range(PARTS):
            out = proj(hid, wd[:, i * cols:(i + 1) * cols])
            back.append(lax.all_to_all(out, axes, 0, 0, tiled=True))

        o = attention(ci.reshape(1), q, kv, c, s, ncp)
        y = (x.astype(F32) + proj(o, wo).astype(F32)).astype(BF16)
        z = rms_norm(y, g_ffn)
        wide = (jax.nn.silu(jnp.dot(z, w1, preferred_element_type=F32)) * jnp.dot(z, w3, preferred_element_type=F32)).astype(BF16)
        f = proj(wide, w2)

        gate, f = lax.optimization_barrier((gate, f))
        w = weigh(gate, ex, cap)
        h = ()
        for i in range(PARTS):
            h = (combine(back[i], w, zero, u, y, f, 16 * cap, i, h),)
        h = h[0]
        return h.reshape(bd, sd, d)

    return jax.shard_map(body, mesh=mesh, in_specs=(tok, tok, rep, rep, rep, rep, rep, rep, rep, rep, rep, rep, rep, exs, exs, exs), out_specs=tok, check_vma=False)
```
